32 devices in a mesh: pipe: 4 (over x, core), vocab: 8 (over z, y).
Axes of the slice: x: 2, y: 2, z: 4, core: 2. Of those that a mesh axis runs over, the one named last changes fastest.
Arguments:
- hidden: bfloat16 [4, 128, 4096], P('pipe'), may hold values from -60 to 60
- norm_gain: float32 [4096], replicated, may hold values from 0.5 to 1.5
- out_weight: bfloat16 [128256, 4096], P(('pipe', 'vocab')), may hold values from -4 to 4
- targets: int32 [4, 128], P('pipe'), may hold values from 0 to 128255
- loss_mask: int32 [4, 128], P('pipe'), may hold values from 0 to 1, as said below
- slot_position: int32 [4, 128], P('pipe'), may hold values from 0 to 127, each once within a row
- counts: int32 [4], replicated, may hold values from 1 to 128, 320 in all
- loss_scale: float32 [], replicated, may hold values from 4096 to 32768
Outputs:
- loss: float32 [], replicated
- grad_hidden: bfloat16 [4, 128, 4096], P('pipe')
The draws below stay inside these ranges and needn't reach their ends.
Inputs may be any that keep to these rules, and one draw needn't show every extreme that they name: The 4 counts sum to exactly 320, and one of them equals 128. Each row of slot_position holds every number of 0 to 127 once. Each row of loss_mask holds at least 64 ones.
All inputs are finite; a program needn't handle non-finite values.
Results may differ from the reference program's by a relative error of at most 0.0034.
Values may be sent and summed in bfloat16 or wider, within the bound.
A program may use at most 128 MiB of HBM per device.

```python
import math
import jax
import jax.numpy as jnp
import numpy as np
from jax import lax

D = 4096
VOCAB = 128256
TOK_MB = 128
MICRO = 4
LIVE = 320


def make_hidden(key):
    folded = jax.random.fold_in(key, 11)
    key_scale, key_noise = jax.random.split(folded)
    scales = jnp.exp(jax.random.uniform(key_scale, (MICRO, TOK_MB, 1), jnp.float32) * math.log(10.0))
    raw_noise = jnp.clip(jax.random.normal(key_noise, (MICRO, TOK_MB, D), jnp.float32), -6.0, 6.0)
    return raw_noise * scales


def draw_hidden(key, part):
    return make_hidden(key).astype(jnp.bfloat16)


def draw_out_weight(key, part):
    folded = jax.random.fold_in(key, 23)
    key_weight = jax.random.fold_in(folded, 0)
    weight = jnp.clip(jax.random.normal(key_weight, (VOCAB, D), jnp.float32), -6.0, 6.0) * (3.0 / math.sqrt(D))
    return weight.astype(jnp.bfloat16)


def draw_loss_mask(key, part):
    folded = jax.random.fold_in(key, 37)
    key_count, key_order = jax.random.split(folded)
    ones_count = jax.random.randint(key_count, (MICRO, 1), TOK_MB // 2, TOK_MB + 1)
    order_keys = jax.random.split(key_order, MICRO)
    ranks = jax.vmap(lambda one_key: jax.random.permutation(one_key, TOK_MB))(order_keys)
    return jnp.where(ranks < ones_count, 1, 0).astype(jnp.int32)


def place_ends(entries, rng, low, largest):
    longest = entries.shape.index(max(entries.shape))
    spots = []
    for shift in (0, 1):
        where = [jax.random.randint(jax.random.fold_in(rng, axis), (), 0, length) for axis, length in enumerate(entries.shape)]
        where[longest] = (where[longest] + shift) % entries.shape[longest]
        spots.append(tuple(where))
    return entries.at[spots[0]].set(low).at[spots[1]].set(largest)


def ranked_wide(own_key, shape, count, lean):
    weights = [min(1 << octave, count + 1 - (1 << octave)) * (1 << 20) // math.isqrt((1 << octave) ** lean) + 1 for octave in range((count + 1).bit_length()) if 1 << octave <= count]
    spread = 1 + sum(weights) // (1 << 30)
    table = np.cumsum(np.array([max(1, weight // spread) for weight in weights]))
    lot = jax.random.randint(jax.random.fold_in(own_key, 1), shape, 0, int(table[len(weights) - 1]))
    start = jnp.left_shift(1, jnp.searchsorted(jnp.asarray(table, jnp.int32), lot, side="right").astype(jnp.int32))
    standing = start - 1 + jax.random.randint(jax.random.fold_in(own_key, 4), shape, 0, 1 << 30) % jnp.minimum(start, count + 1 - start)
    return jax.random.permutation(jax.random.fold_in(own_key, 2), count)[standing].astype(jnp.int32)


def length_profile(amount, total, bound, skew):
    weights = [(1 << 20) // math.isqrt(rank ** skew) + 1 for rank in range(2, amount + 1)]
    spare, holding = total - bound - (amount - 1), [1] * (amount - 1)
    while spare > 0:
        movable = [i for i in range(amount - 1) if holding[i] < bound]
        whole, left = sum([weights[i] for i in movable]), spare
        for i in movable:
            addition = min(bound - holding[i], max(1, left * weights[i] // whole), spare)
            holding[i] = holding[i] + addition
            spare = spare - addition
    return np.array([bound] + holding)


def uneven_parts(own_key, number_of, total, reach, lean):
    if number_of == 2:
        one = jax.random.randint(own_key, (), max(1, total - reach), min(reach, total - 1) + 1)
        return jnp.stack([one, total - one])
    sizes = jnp.asarray(length_profile(number_of, total, reach, lean), jnp.int32)
    couples = (number_of - 1) // 2
    donor, sink = sizes[1:1 + 2 * couples:2], sizes[2:2 + 2 * couples:2]
    margin = jnp.minimum(donor - 1, reach - sink)
    shifted = jax.random.randint(jax.random.fold_in(own_key, 1), (couples,), 0, 1 << 20) % (margin + 1)
    sizes = sizes.at[1:1 + 2 * couples:2].set(donor - shifted).at[2:2 + 2 * couples:2].set(sink + shifted)
    return sizes[jax.random.permutation(jax.random.fold_in(own_key, 2), number_of)]


def setup_inputs(seed: int = 0) -> dict:
    seeds = jax.random.split(jax.random.key(seed), 9)
    return {
        "hidden": draw_hidden(jax.random.fold_in(seeds[8], 71), 0),
        "norm_gain": jnp.clip(1.0 + 0.1 * jax.random.normal(seeds[1], (D,), jnp.float32), 0.5, 1.5),
        "out_weight": draw_out_weight(jax.random.fold_in(seeds[8], 71), 0),
        "targets": place_ends(ranked_wide(seeds[3], (MICRO, TOK_MB), VOCAB, 2), jax.random.fold_in(seeds[3], 3), 0, VOCAB - 1).astype(jnp.int32),
        "loss_mask": draw_loss_mask(jax.random.fold_in(seeds[8], 71), 0),
        "slot_position": jax.vmap(lambda own: jax.random.permutation(own, TOK_MB))(jax.random.split(seeds[5], MICRO)).reshape((MICRO, TOK_MB)).astype(jnp.int32),
        "counts": uneven_parts(seeds[6], MICRO, LIVE, TOK_MB, 2).astype(jnp.int32),
        "loss_scale": jnp.clip(jnp.exp(jax.random.uniform(seeds[7], (), jnp.float32, math.log(4096.0), math.log(32768.0))), 4096.0, 32768.0),
    }


EPSILON = 1e-05

def rms_scale(values, norm_gain):
    mean_square = lax.optimization_barrier(jnp.mean(values * values, axis=-1, keepdims=True))
    return values * lax.rsqrt(mean_square + EPSILON) * norm_gain.astype(jnp.float32)

def micro_terms(normed_rows, target_row, weight_row, out_weight, loss_scale, weight_total):
    logits = lax.dot_general(normed_rows, out_weight, (((1,), (1,)), ((), ())), preferred_element_type=jnp.float32)
    row_top = lax.optimization_barrier(jnp.max(logits, axis=1))
    exp_total = lax.optimization_barrier(jnp.sum(jnp.exp(logits - row_top[:, None]), axis=1))
    log_total = row_top + jnp.log(exp_total)
    is_target = jnp.arange(VOCAB, dtype=jnp.int32)[None, :] == target_row.astype(jnp.int32)[:, None]
    target_logit = lax.optimization_barrier(jnp.sum(jnp.where(is_target, logits, 0.0), axis=1))
    loss_part = jnp.sum(weight_row * (log_total - target_logit))
    token_coef = loss_scale * weight_row / weight_total
    logit_grad = ((jnp.exp(logits - log_total[:, None]) - is_target.astype(jnp.float32)) * token_coef[:, None]).astype(jnp.bfloat16)
    normed_grad = jnp.dot(logit_grad, out_weight, preferred_element_type=jnp.float32)
    return (loss_part, normed_grad)

def reference(hidden, norm_gain, out_weight, targets, loss_mask, slot_position, counts, loss_scale):
    rows_total = MICRO * TOK_MB
    flat = hidden.reshape(rows_total, D).astype(jnp.float32)
    normed = rms_scale(flat, norm_gain).astype(jnp.bfloat16)
    inside = slot_position < counts[:, None]
    token_weight = jnp.where(inside & (loss_mask == 1), 1.0, 0.0).astype(jnp.float32)
    weight_total = jnp.sum(token_weight)

    def one_micro(item):
        return micro_terms(item[0], item[1], item[2], out_weight, loss_scale, weight_total)
    loss_parts, normed_grad = lax.map(one_micro, (normed.reshape(MICRO, TOK_MB, D), targets, token_weight))
    loss = jnp.sum(loss_parts) / weight_total
    pullback = jax.vjp(lambda values: rms_scale(values, norm_gain), flat)[1]
    grad_flat = pullback(normed_grad.reshape(rows_total, D))[0]
    return (loss, grad_flat.astype(jnp.bfloat16).reshape(MICRO, TOK_MB, D))
```

```python
import functools
import jax
import jax.numpy as jnp
from jax import lax
from jax.experimental import pallas as pl
from jax.experimental.pallas import tpu as pltpu
from jax.sharding import PartitionSpec as P

EPSILON = 1e-05
MESH = pl.DeviceIdType.MESH
F32 = jnp.float32
BF16 = jnp.bfloat16
VMEM = pl.BlockSpec(memory_space=pltpu.VMEM)


def rms_scale(values, norm_gain):
    mean_square = jnp.mean(values * values, axis=-1, keepdims=True)
    return values * lax.rsqrt(mean_square + EPSILON) * norm_gain


def pull_rows(rows, norm_gain, cotangent):
    pullback = jax.vjp(lambda values: rms_scale(values, norm_gain), rows)[1]
    return pullback(cotangent)[0].astype(BF16)


def place(ny):
    p, v = lax.axis_index("pipe"), lax.axis_index("vocab")
    return p // 2, p % 2, v % ny, v // ny


def greet(targets):
    barrier = pltpu.get_barrier_semaphore()
    for target in targets:
        pl.semaphore_signal(barrier, inc=1, device_id=target, device_id_type=MESH)
    pl.semaphore_wait(barrier, len(targets))


def remote(src, dst, send, recv, target):
    return pltpu.make_async_remote_copy(
        src_ref=src, dst_ref=dst, send_sem=send, recv_sem=recv,
        device_id=target, device_id_type=MESH,
    )


LIVE_SHARE = 80
F_MIN = -1e30


def flip(i, by):
    return i + by * (1 - 2 * i)


def lanes_of(col):
    rows, lanes = col.shape
    outs = []
    for b in range(0, rows, lanes):
        part = col[b:min(b + lanes, rows)]
        r = lax.broadcasted_iota(jnp.int32, part.shape, 0)
        l = lax.broadcasted_iota(jnp.int32, part.shape, 1)
        outs.append(jnp.sum(jnp.where(r == l, part, 0.0), axis=0, keepdims=True))
    return outs


def col_of(row, count):
    shape = (count, row.shape[1])
    r = lax.broadcasted_iota(jnp.int32, shape, 0)
    l = lax.broadcasted_iota(jnp.int32, shape, 1)
    return jnp.sum(jnp.where(r == l, jnp.broadcast_to(row, shape), 0.0), axis=1, keepdims=True)


def gather_kernel(ny, chunks, counts, own, ints, gain, hc, nc, meta, posn, live_out,
                  hall, oints, sel, sems_s, sems_r, own_s, own_r, int_s, int_r):
    x, core, y, z = place(ny)
    p, v = x * 2 + core, z * ny + y
    pipe, slots, width = hall.shape
    part = slots // (2 * chunks)
    mate = (x * 2 + (1 - core), v)
    across = ((1 - x) * 2 + core, v)
    diag = ((1 - x) * 2 + (1 - core), v)
    beside = (p, z * ny + (1 - y))
    greet([mate, across, diag, beside])
    far = (1 - x) * 2 + core
    started = []
    first = []

    def rows(side, c):
        return pl.ds(pl.multiple_of((side * chunks + c) * part, part), part)

    for c in range(chunks):
        cp = remote(own.at[rows(y, c)], hall.at[p, rows(y, c)], sems_s.at[0, c], sems_r.at[0, c], across)
        cp.start()
        first.append(cp)
    for j, target in enumerate((mate, across, diag)):
        cp = remote(ints, oints.at[p], int_s.at[j], int_r.at[j], target)
        cp.start()
        started.append(cp)
    cp = remote(own, hall.at[p], own_s, own_r, mate)
    cp.start()
    started.append(cp)
    oints[p] = ints[...]
    hall[p] = own[...]
    second = []
    for c in range(chunks):
        first[c].wait_recv()
        cy = remote(hall.at[far, rows(y, c)], hall.at[far, rows(y, c)], sems_s.at[1, c], sems_r.at[1, c], beside)
        cy.start()
        cm = remote(hall.at[far, rows(y, c)], hall.at[far, rows(y, c)], sems_s.at[2, c], sems_r.at[2, c], mate)
        cm.start()
        second.append(cy)
        started.append(cm)
    for c in range(chunks):
        second[c].wait_recv()
        cm = remote(hall.at[far, rows(1 - y, c)], hall.at[far, rows(1 - y, c)], sems_s.at[3, c], sems_r.at[3, c], mate)
        cm.start()
        started.append(cm)
    for cp in started:
        cp.wait_recv()

    bound = hc.shape[0]
    square = (slots, slots)
    r0 = lax.broadcasted_iota(jnp.int32, square, 0)
    l0 = lax.broadcasted_iota(jnp.int32, square, 1)
    ri = lax.broadcasted_iota(jnp.int32, (bound, slots), 0).astype(F32)
    base = jnp.zeros((1, 1), F32)
    tgt = jnp.zeros((bound, 1), F32)
    for m in range(pipe):
        inside = oints[m, 2:3, :] < counts[m]
        live = jnp.where(inside & (oints[m, 1:2, :] == 1), 1.0, 0.0).astype(F32)
        live_sq = jnp.broadcast_to(live, square)
        col_live = jnp.sum(jnp.where(r0 == l0, live_sq, 0.0), axis=1, keepdims=True)
        pos_col = jnp.sum(jnp.where(l0 < r0, live_sq, 0.0), axis=1, keepdims=True) + base
        pos_row = jnp.sum(jnp.where(r0 < l0, jnp.broadcast_to(col_live, square), 0.0), axis=0, keepdims=True) + base
        one = jnp.where((ri == jnp.broadcast_to(pos_row, ri.shape))
                        & (jnp.broadcast_to(live, ri.shape) == 1.0), 1.0, 0.0)
        sel[:, m * slots:(m + 1) * slots] = one.astype(BF16)
        tgt = tgt + jnp.sum(one * oints[m, 0:1, :].astype(F32), axis=1, keepdims=True)
        posn[m] = jnp.broadcast_to(jnp.where(col_live == 1.0, pos_col, -1.0), posn.shape[1:])
        base = base + jnp.sum(live, axis=1, keepdims=True)
    live_out[...] = jnp.broadcast_to(base, live_out.shape)
    lane = (bound, meta.shape[2])
    meta[0] = jnp.broadcast_to(tgt, lane)
    rl = lax.broadcasted_iota(jnp.int32, lane, 0).astype(F32)
    meta[1] = jnp.where(rl < jnp.broadcast_to(base, lane), 1.0, 0.0)
    meta[2] = jnp.zeros(lane, F32)
    step = 512

    def compact(c, carry):
        cols = pl.ds(pl.multiple_of(c * step, step), step)
        block = hall[:, :, cols].reshape(pipe * slots, step)
        h = jnp.dot(sel[...], block, preferred_element_type=F32)
        hc[:, cols] = h.astype(BF16)
        sq = h * h
        acc = meta[2]
        for k in range(0, step, lane[1]):
            acc = acc + sq[:, k:k + lane[1]]
        meta[2] = acc
        return carry
    lax.fori_loop(0, width // step, compact, 0)
    mean = jnp.sum(meta[2], axis=1, keepdims=True) / width
    meta[2] = jnp.broadcast_to(lax.rsqrt(mean + EPSILON), lane)

    def norm(c, carry):
        cols = pl.ds(pl.multiple_of(c * lane[1], lane[1]), lane[1])
        nc[:, cols] = (hc[:, cols].astype(F32) * meta[2] * gain[:, cols]).astype(BF16)
        return carry
    lax.fori_loop(0, width // lane[1], norm, 0)
    for cp in first + second + started:
        cp.wait_send()


def gather(hidden, ints, counts, gain, pipe, ny, chunks, bound):
    slots, width = hidden.shape
    dma = pltpu.SemaphoreType.DMA
    return pl.pallas_call(
        functools.partial(gather_kernel, ny, chunks),
        out_shape=(
            jax.ShapeDtypeStruct((bound, width), BF16),
            jax.ShapeDtypeStruct((bound, width), BF16),
            jax.ShapeDtypeStruct((3, bound, 128), F32),
            jax.ShapeDtypeStruct((pipe, slots, 128), F32),
            jax.ShapeDtypeStruct((8, 128), F32),
        ),
        in_specs=[pl.BlockSpec(memory_space=pltpu.SMEM), VMEM, VMEM, VMEM],
        out_specs=(VMEM,) * 5,
        scratch_shapes=[
            pltpu.VMEM((pipe, slots, width), BF16),
            pltpu.VMEM((pipe,) + ints.shape, jnp.int32),
            pltpu.VMEM((bound, pipe * slots), BF16),
            dma((4, chunks)), dma((4, chunks)), dma, dma, dma((3,)), dma((3,)),
        ],
        compiler_params=pltpu.CompilerParams(
            collective_id=0, has_side_effects=True, vmem_limit_bytes=24 * 2**20
        ),
    )(counts, hidden, ints, gain)


def head_kernel(pipe, vocab, ny, words, scale_ref, weight, nc, hc, meta, posn, live, gain,
                out, loss, wv, lg, gb, mx, tg, st, box, st2, box2, ms, ob, mr, sb, rb, own, zs, zr, ag,
                w_sem, st_s, st_r, s2_s, s2_r, m_s, m_r, x_s, x_r, z_s, z_r, az_s, az_r,
                ax_s, ax_r, am_s, am_r):
    x, core, y, z = place(ny)
    p, v = x * 2 + core, z * ny + y
    nz = vocab // ny
    rows, width = nc.shape
    padded = wv.shape[0]
    tile = 512
    tiles = padded // tile
    rest = words - (tiles - 1) * tile
    lane = (rows, 128)
    offset = (p * vocab + v) * words

    def load(t):
        size = tile if t < tiles - 1 else rest
        return pltpu.make_async_copy(
            weight.at[pl.ds(t * tile, size)], wv.at[pl.ds(t * tile, size)], w_sem.at[t])

    for t in range(tiles - 1):
        load(t).start()
    edge = words // 16 * 16
    wv[edge:, :] = jnp.zeros((padded - edge, width), BF16)
    load(tiles - 1).start()

    peers = []
    for dp in range(pipe):
        for dv in range(vocab):
            if dp or dv:
                peers.append((lax.rem(p + dp, pipe), lax.rem(v + dv, vocab)))
    greet(peers)
    copies = []

    def go(src, dst, send, recv, target):
        cp = remote(src, dst, send, recv, target)
        cp.start()
        copies.append(cp)
        return cp

    mx[...] = jnp.full(lane, F_MIN, F32)
    tg[...] = jnp.zeros(lane, F32)

    def forward(t, carry):
        @pl.when(t < tiles - 1)
        def _():
            pltpu.make_async_copy(
                weight.at[pl.ds(pl.multiple_of(t * tile, tile), tile)],
                wv.at[pl.ds(pl.multiple_of(t * tile, tile), tile)], w_sem.at[t]).wait()

        @pl.when(t == tiles - 1)
        def _():
            load(tiles - 1).wait()
        wt = wv[pl.ds(pl.multiple_of(t * tile, tile), tile), :]
        logit = lax.dot_general(nc[...], wt, (((1,), (1,)), ((), ())), preferred_element_type=F32)
        col = lax.broadcasted_iota(jnp.int32, (1, 128), 1)
        top, hit = mx[...], tg[...]
        want = meta[0] - (offset + t * tile).astype(F32)
        for k in range(tile // 128):
            here = col + k * 128
            part = jnp.where(here + t * tile < words, logit[:, k * 128:(k + 1) * 128], F_MIN)
            lg[:, pl.ds(pl.multiple_of(t * tile + k * 128, 128), 128)] = part
            top = jnp.maximum(top, part)
            hit = hit + jnp.where((want == here.astype(F32)) & (part > F_MIN), part, 0.0)
        mx[...] = top
        tg[...] = hit
        return carry
    lax.fori_loop(0, tiles, forward, 0)

    top = jnp.max(mx[...], axis=1, keepdims=True)
    hit = jnp.sum(tg[...], axis=1, keepdims=True)
    mx[...] = jnp.broadcast_to(top, lane)
    tg[...] = jnp.zeros(lane, F32)
    blk = 64

    def expsum(t, carry):
        for b in range(0, rows, blk):
            ref = mx[b:b + blk]
            acc = tg[b:b + blk]
            for k in range(tile // 128):
                acc = acc + jnp.exp(lg[b:b + blk, pl.ds(pl.multiple_of(t * tile + k * 128, 128), 128)] - ref)
            tg[b:b + blk] = acc
        return carry
    lax.fori_loop(0, tiles, expsum, 0)
    part_lse = top + jnp.log(jnp.sum(tg[...], axis=1, keepdims=True))
    groups = -(-rows // 128)
    st[...] = jnp.zeros(st.shape, F32)
    for i, piece in enumerate(lanes_of(jnp.broadcast_to(part_lse, lane))):
        st[i:i + 1, :] = piece
    for i, piece in enumerate(lanes_of(jnp.broadcast_to(hit, lane))):
        st[groups + i:groups + i + 1, :] = piece
    stats = [go(st, box.at[j], st_s.at[j], st_r.at[j], t) for j, t in enumerate(peers)]
    for cp in stats:
        cp.wait_recv()
    mine = st[...]
    best = jnp.maximum(mine, jnp.max(box[...], axis=0))
    total = jnp.exp(mine - best) + jnp.sum(jnp.exp(box[...] - best[None]), axis=0)
    lse = best + jnp.log(total)
    target = mine + jnp.sum(box[...], axis=0)
    count = live[0:1, :]
    missing = jnp.zeros((1, 128), F32)
    for i in range(groups):
        at = (lax.broadcasted_iota(jnp.int32, (1, 128), 1) + i * 128).astype(F32)
        missing = missing + jnp.where(at < count, lse[i:i + 1] - target[groups + i:groups + i + 1], 0.0)
    loss[...] = jnp.broadcast_to(jnp.sum(missing, axis=1, keepdims=True) / count, loss.shape)
    for i in range(groups):
        size = min(128, rows - i * 128)
        mx[i * 128:i * 128 + size] = jnp.broadcast_to(col_of(lse[i:i + 1], size), (size, 128))
    tg[...] = jnp.zeros(lane, F32)
    coef = scale_ref[0] / count

    def logit_grad(t, carry):
        for b in range(0, rows, blk):
            ref = mx[b:b + blk]
            factor = coef * meta[1, b:b + blk]
            want = meta[0, b:b + blk] - (offset + t * tile).astype(F32)
            acc = tg[b:b + blk]
            for k in range(tile // 128):
                cols = pl.ds(pl.multiple_of(t * tile + k * 128, 128), 128)
                l = lg[b:b + blk, cols]
                here = (lax.broadcasted_iota(jnp.int32, (1, 128), 1) + k * 128).astype(F32)
                hot = jnp.where((want == here) & (l > F_MIN), 1.0, 0.0)
                g = ((jnp.exp(l - ref) - hot) * factor).astype(BF16)
                gb[b:b + blk, cols] = g
                acc = acc + g.astype(F32) * l
            tg[b:b + blk] = acc
        return carry
    lax.fori_loop(0, tiles, logit_grad, 0)
    st2[...] = jnp.zeros(st2.shape, F32)
    for i, piece in enumerate(lanes_of(jnp.broadcast_to(jnp.sum(tg[...], axis=1, keepdims=True), lane))):
        st2[i:i + 1, :] = piece
    dots = [go(st2, box2.at[j], s2_s.at[j], s2_r.at[j], t) for j, t in enumerate(peers)]

    steps = width // (2 * tile)
    kb = tile // 128
    zrows = rows // nz
    mate = (x * 2 + (1 - core), v)
    spot = x * ny + y
    near = []
    for q in range(1, 4):
        tx, ty = flip(x, q // 2), flip(y, q % 2)
        near.append(((tx * 2 + core, z * ny + ty), tx * ny + ty))
    along = [(p, lax.rem(z + d, nz) * ny + y) for d in range(1, nz)]
    to_mate, to_near, to_z, ag_z, ag_x, ag_m = {}, {}, {}, {}, {}, {}

    def product(j, dst):
        acc = jnp.dot(gb[...], wv[:, pl.ds(pl.multiple_of(j * tile, tile), tile)],
                      preferred_element_type=F32)
        for k in range(kb):
            dst[k] = acc[:, k * 128:(k + 1) * 128]

    def for_mate(s):
        if s >= 2:
            to_mate[s - 2].wait_send()
        product(2 * s + (1 - core), ms.at[s % 2])
        to_mate[s] = remote(ms.at[s % 2], mr.at[s], m_s.at[s], m_r.at[s], mate)
        to_mate[s].start()

    def for_self(s):
        product(2 * s + core, ob)
        to_mate[s].wait_recv()
        for q, (target_id, block) in enumerate(near):
            sb[s, q] = (ob[block] + mr[s, block]).astype(BF16)
            to_near[s, q] = go(sb.at[s, q], rb.at[s, q], x_s.at[s, q], x_r.at[s, q], target_id)
        own[s] = ob[spot] + mr[s, spot]

    def plane(s):
        for q in range(3):
            to_near[s, q].wait_recv()
        own[s] = own[s] + (rb[s, 0].astype(F32) + rb[s, 1].astype(F32) + rb[s, 2].astype(F32))
        for d in range(1, nz):
            zz = lax.rem(z + d, nz)
            zs[s, d - 1] = own[s, pl.ds(pl.multiple_of(zz * zrows, 16), zrows)].astype(BF16)
            to_z[s, d] = go(zs.at[s, d - 1], zr.at[s, d - 1], z_s.at[s, d - 1], z_r.at[s, d - 1], along[d - 1])

    mine_rows = pl.ds(pl.multiple_of(z * zrows, 16), zrows)

    def row_dots():
        for cp in dots:
            cp.wait_recv()
        full = st2[...] + jnp.sum(box2[...], axis=0)
        for i in range(groups):
            size = min(128, rows - i * 128)
            tg[i * 128:i * 128 + size] = jnp.broadcast_to(col_of(full[i:i + 1], size), (size, 128))

    def finish(s):
        for d in range(1, nz):
            to_z[s, d].wait_recv()
        g = own[s, mine_rows]
        for d in range(1, nz):
            g = g + zr[s, d - 1].astype(F32)
        cols = pl.ds(pl.multiple_of((2 * s + core) * tile + spot * 128, 128), 128)
        r = meta[2, mine_rows]
        h = hc[mine_rows, cols].astype(F32)
        value = r * (gain[:, cols] * g) - (r * r) * h * (tg[mine_rows] * (1.0 / width))
        ag[core, spot, s, z] = value.astype(BF16)
        for d in range(1, nz):
            piece = ag.at[core, spot, s, z]
            ag_z[s, d] = go(piece, piece, az_s.at[s, d - 1], az_r.at[s, d - 1], along[d - 1])

    def spread(s):
        for d in range(1, nz):
            ag_z[s, d].wait_recv()
        piece = ag.at[core, spot, s]
        for q, (target_id, block) in enumerate(near):
            ag_x[s, q] = go(piece, piece, ax_s.at[s, q], ax_r.at[s, q], target_id)
        ag_m[s, 3] = go(piece, piece, am_s.at[s, 3], am_r.at[s, 3], mate)

    def share(s):
        for q, (target_id, block) in enumerate(near):
            ag_x[s, q].wait_recv()
            piece = ag.at[core, block, s]
            ag_m[s, q] = go(piece, piece, am_s.at[s, q], am_r.at[s, q], mate)

    def scatter(s):
        for q in range(4):
            ag_m[s, q].wait_recv()
        slots = out.shape[0]
        at = lax.broadcasted_iota(jnp.int32, (slots, rows), 1).astype(F32)
        back = jnp.where(at == jnp.broadcast_to(posn[p, :, 0:1], (slots, rows)), 1.0, 0.0).astype(BF16)
        for c in range(2):
            block = jnp.concatenate([ag[c, k, s].reshape(rows, 128) for k in range(kb)], axis=1)
            res = jnp.dot(back, block, preferred_element_type=F32).astype(BF16)
            out[:, (2 * s + c) * tile:(2 * s + c + 1) * tile] = res

    for s in range(steps):
        for_mate(s)
        if s >= 2:
            plane(s - 2)
        if s == 2:
            row_dots()
        if s >= 3:
            finish(s - 3)
        for_self(s)
    order = []
    for i in range(steps + 6):
        for lag, f in ((0, plane), (1, finish), (2, spread), (3, share), (4, scatter)):
            s = i + steps - 2 - lag
            if 0 <= s < steps and not (f is finish and s <= steps - 4):
                order.append((f, s))
    for f, s in order:
        f(s)
    for s in range(max(steps - 2, 0), steps):
        to_mate[s].wait_send()
    for cp in copies:
        cp.wait_send()


def head(nc, hc, meta, posn, live, norm_gain, out_weight, loss_scale, pipe, vocab, ny, slots):
    rows, width = nc.shape
    words = out_weight.shape[0]
    padded = -(-words // 512) * 512
    nz = vocab // ny
    steps = width // 1024
    n = pipe * vocab - 1
    zrows = rows // nz
    dma = pltpu.SemaphoreType.DMA
    vm = pltpu.VMEM
    return pl.pallas_call(
        functools.partial(head_kernel, pipe, vocab, ny, words),
        out_shape=(
            jax.ShapeDtypeStruct((slots, width), BF16),
            jax.ShapeDtypeStruct((8, 128), F32),
        ),
        in_specs=[pl.BlockSpec(memory_space=pltpu.SMEM), pl.BlockSpec(memory_space=pl.ANY)] + [VMEM] * 6,
        out_specs=(VMEM, VMEM),
        scratch_shapes=[
            vm((padded, width), BF16),
            vm((rows, padded), F32),
            vm((rows, padded), BF16),
            vm((rows, 128), F32), vm((rows, 128), F32),
            vm((8, 128), F32), vm((n, 8, 128), F32),
            vm((8, 128), F32), vm((n, 8, 128), F32),
            vm((2, 4, rows, 128), F32),
            vm((4, rows, 128), F32),
            vm((steps, 4, rows, 128), F32),
            vm((steps, 3, rows, 128), BF16),
            vm((steps, 3, rows, 128), BF16),
            vm((steps, rows, 128), F32),
            vm((steps, nz - 1, zrows, 128), BF16),
            vm((steps, nz - 1, zrows, 128), BF16),
            vm((2, 4, steps, nz, zrows, 128), BF16),
            dma((padded // 512,)),
            dma((n,)), dma((n,)), dma((n,)), dma((n,)),
            dma((steps,)), dma((steps,)),
            dma((steps, 3)), dma((steps, 3)),
            dma((steps, nz - 1)), dma((steps, nz - 1)),
            dma((steps, nz - 1)), dma((steps, nz - 1)),
            dma((steps, 3)), dma((steps, 3)),
            dma((steps, 4)), dma((steps, 4)),
        ],
        compiler_params=pltpu.CompilerParams(
            collective_id=1, has_side_effects=True, vmem_limit_bytes=62 * 2**20
        ),
    )(loss_scale.reshape(1), out_weight, nc, hc, meta, posn, live, norm_gain.reshape(1, width))


def body(pipe, vocab, hidden, norm_gain, out_weight, targets, loss_mask, slot_position, counts, loss_scale):
    micro_slots = hidden.shape[1]
    model_width = hidden.shape[2]
    shard_words = out_weight.shape[0]
    ny = 2
    nz = vocab // ny
    fast = (pipe == 4 and vocab == 8 and micro_slots == 128 and model_width % 1024 == 0
            and shard_words % 8 == 0)
    own_ints = jnp.concatenate(
        [targets, loss_mask, slot_position, jnp.zeros((5, micro_slots), jnp.int32)], axis=0
    )
    if fast:
        hc, nc, meta, posn, live = gather(
            hidden.reshape(micro_slots, model_width), own_ints, counts,
            norm_gain.reshape(1, model_width), pipe, ny, 4, LIVE_SHARE * pipe)
        grad_out, loss = head(nc, hc, meta, posn, live, norm_gain, out_weight, loss_scale,
                              pipe, vocab, ny, micro_slots)
        return (loss[0, 0], grad_out.reshape(1, micro_slots, model_width))
    offset = lax.axis_index(("pipe", "vocab")) * shard_words
    own_rows = hidden.reshape(micro_slots, model_width).astype(F32)
    own_normed = rms_scale(own_rows, norm_gain).astype(BF16)
    all_normed = lax.all_gather(own_normed, "pipe", axis=0, tiled=True)
    all_ints = lax.all_gather(own_ints, "pipe", axis=0)
    rows_total = all_normed.shape[0]
    all_targets, all_masks, all_positions = (
        all_ints[:, k].reshape(rows_total) for k in range(3)
    )
    count_row = jnp.broadcast_to(counts[:, None], (counts.shape[0], micro_slots)).reshape(rows_total)
    inside = all_positions < count_row
    token_weight = jnp.where(inside & (all_masks == 1), 1.0, 0.0).astype(F32)
    weight_total = jnp.sum(token_weight)
    logits = lax.dot_general(
        all_normed, out_weight, (((1,), (1,)), ((), ())), preferred_element_type=F32
    )
    is_target = (
        jnp.arange(shard_words, dtype=jnp.int32)[None, :] == (all_targets - offset)[:, None]
    )
    local_target = jnp.sum(jnp.where(is_target, logits, 0.0), axis=1)
    local_top = jnp.max(logits, axis=1)
    row_top = lax.pmax(local_top, ("pipe", "vocab"))
    local_total = jnp.sum(jnp.exp(logits - row_top[:, None]), axis=1)
    exp_total, target_logit = lax.psum((local_total, local_target), ("pipe", "vocab"))
    log_total = row_top + jnp.log(exp_total)
    loss = jnp.sum(token_weight * (log_total - target_logit)) / weight_total
    token_coef = loss_scale * token_weight / weight_total
    logit_grad = (
        (jnp.exp(logits - log_total[:, None]) - is_target.astype(F32)) * token_coef[:, None]
    ).astype(BF16)
    work_grad = jnp.dot(logit_grad, out_weight, preferred_element_type=F32)
    grad_cube = work_grad.reshape(rows_total // micro_slots, micro_slots, model_width)
    micro_grad = lax.psum_scatter(grad_cube, "pipe", scatter_dimension=0, tiled=True)
    summed = lax.psum(micro_grad, "vocab")
    grad_out = pull_rows(own_rows, norm_gain, summed.reshape(micro_slots, model_width))
    return (loss, grad_out.reshape(1, micro_slots, model_width))


def solution(mesh):
    in_specs = (
        P("pipe", None, None),
        P(),
        P(("pipe", "vocab"), None),
        P("pipe", None),
        P("pipe", None),
        P("pipe", None),
        P(),
        P(),
    )
    out_specs = (P(), P("pipe", None, None))
    part = functools.partial(body, mesh.shape["pipe"], mesh.shape["vocab"])
    return jax.shard_map(part, mesh=mesh, in_specs=in_specs, out_specs=out_specs, check_vma=False)
```

```python
import functools
import jax
import jax.numpy as jnp
from jax import lax
from jax.experimental import pallas as pl
from jax.experimental.pallas import tpu as pltpu
from jax.sharding import PartitionSpec as P

EPSILON = 1e-05
MESH = pl.DeviceIdType.MESH
F32 = jnp.float32
BF16 = jnp.bfloat16
VMEM = pl.BlockSpec(memory_space=pltpu.VMEM)


def rms_scale(values, norm_gain):
    mean_square = jnp.mean(values * values, axis=-1, keepdims=True)
    return values * lax.rsqrt(mean_square + EPSILON) * norm_gain


def pull_rows(rows, norm_gain, cotangent):
    pullback = jax.vjp(lambda values: rms_scale(values, norm_gain), rows)[1]
    return pullback(cotangent)[0].astype(BF16)


def place(ny):
    p, v = lax.axis_index("pipe"), lax.axis_index("vocab")
    return p // 2, p % 2, v % ny, v // ny


def greet(targets):
    barrier = pltpu.get_barrier_semaphore()
    for target in targets:
        pl.semaphore_signal(barrier, inc=1, device_id=target, device_id_type=MESH)
    pl.semaphore_wait(barrier, len(targets))


def remote(src, dst, send, recv, target):
    return pltpu.make_async_remote_copy(
        src_ref=src, dst_ref=dst, send_sem=send, recv_sem=recv,
        device_id=target, device_id_type=MESH,
    )


LIVE_SHARE = 80
F_MIN = -1e30


def flip(i, by):
    return i + by * (1 - 2 * i)


def lanes_of(col):
    rows, lanes = col.shape
    outs = []
    for b in range(0, rows, lanes):
        part = col[b:min(b + lanes, rows)]
        r = lax.broadcasted_iota(jnp.int32, part.shape, 0)
        l = lax.broadcasted_iota(jnp.int32, part.shape, 1)
        outs.append(jnp.sum(jnp.where(r == l, part, 0.0), axis=0, keepdims=True))
    return outs


def col_of(row, count):
    shape = (count, row.shape[1])
    r = lax.broadcasted_iota(jnp.int32, shape, 0)
    l = lax.broadcasted_iota(jnp.int32, shape, 1)
    return jnp.sum(jnp.where(r == l, jnp.broadcast_to(row, shape), 0.0), axis=1, keepdims=True)


def head_kernel(pipe, vocab, ny, words, counts, scale_ref, hidden, targets, masks, places, gain_hbm, weight,
                out, loss, wv, lg, buf, sel, back, ti, gain, meta, live, hsel, mx, tg, sm,
                st, box, st2, box2, mr, sb, rb, own, zs, zr, ag,
                w_sem, o_sem, i_sem, f_s, f_r, n_s, n_r, c_s, c_r, d_s, d_r, e_s, e_r, t_s, t_r,
                st_s, st_r, s2_s, s2_r, m_s, m_r, x_s, x_r, z_s, z_r, az_s, az_r,
                ax_s, ax_r, am_s, am_r):
    x, core, y, z = place(ny)
    p, v = x * 2 + core, z * ny + y
    nz = vocab // ny
    slots, width = hidden.shape
    half = slots // 2
    rows = buf.shape[0]
    padded = wv.shape[0]
    tile = 512
    tiles = padded // tile
    rest = words - (tiles - 1) * tile
    lane = (rows, 128)
    offset = (p * vocab + v) * words
    chunks = width // tile
    far = 1 - x
    mate = (x * 2 + (1 - core), v)
    across = ((1 - x) * 2 + core, v)
    diag = ((1 - x) * 2 + (1 - core), v)
    beside = (p, z * ny + (1 - y))
    copies = []

    def go(src, dst, send, recv, target):
        cp = remote(src, dst, send, recv, target)
        cp.start()
        copies.append(cp)
        return cp

    def cols_at(c):
        return pl.ds(c * tile, tile)

    pool = (tiles - 1) * tile

    def half_rows(a, side):
        return pl.ds(pl.multiple_of(pool + (a * 2 + core) * slots + side * half, half), half)

    def side_rows(a):
        return pl.ds(pl.multiple_of(pool + a * 2 * slots, slots), 2 * slots)

    all_rows = pl.ds(pl.multiple_of(pool + p * slots, slots), slots)
    bring = [pltpu.make_async_copy(hidden.at[:, cols_at(c)], wv.at[all_rows, cols_at(c)], o_sem.at[c])
             for c in range(chunks)]
    small = [pltpu.make_async_copy(src, ti.at[p, k], i_sem.at[k])
             for k, src in enumerate((targets, masks, places))]
    small.append(pltpu.make_async_copy(gain_hbm, gain, i_sem.at[3]))
    for cp in small + bring:
        cp.start()

    def load(t):
        size = tile if t < tiles - 1 else rest
        return pltpu.make_async_copy(
            weight.at[pl.ds(t * tile, size)], wv.at[pl.ds(t * tile, size)], w_sem.at[t])

    peers = []
    for dp in range(pipe):
        for dv in range(vocab):
            if dp or dv:
                peers.append((lax.rem(p + dp, pipe), lax.rem(v + dv, vocab)))
    greet(peers)

    for cp in small:
        cp.wait()
    info = [go(ti.at[p], ti.at[p], t_s.at[j], t_r.at[j], target)
            for j, target in enumerate((mate, across, diag))]
    first, nigh, cross, second, third = [], [], [], [], []
    for c in range(chunks):
        bring[c].wait()
        piece = wv.at[half_rows(x, y), cols_at(c)]
        first.append(go(piece, piece, f_s.at[c], f_r.at[c], across))
        piece = wv.at[all_rows, cols_at(c)]
        nigh.append(go(piece, piece, n_s.at[c], n_r.at[c], mate))
    for t in range(tiles - 1):
        load(t).start()
    for cp in info:
        cp.wait_recv()

    square = (slots, slots)
    r0 = lax.broadcasted_iota(jnp.int32, square, 0)
    l0 = lax.broadcasted_iota(jnp.int32, square, 1)
    ri = lax.broadcasted_iota(jnp.int32, (rows, slots), 0).astype(F32)
    li = lax.broadcasted_iota(jnp.int32, (slots, rows), 1).astype(F32)
    base = jnp.zeros((1, 1), F32)
    tgt = jnp.zeros((rows, 1), F32)
    for m in range(pipe):
        inside = ti[m, 2] < counts[m]
        alive = jnp.where(inside & (ti[m, 1] == 1), 1.0, 0.0).astype(F32)
        alive_sq = jnp.broadcast_to(alive, square)
        col_live = jnp.sum(jnp.where(r0 == l0, alive_sq, 0.0), axis=1, keepdims=True)
        pos_col = jnp.sum(jnp.where(l0 < r0, alive_sq, 0.0), axis=1, keepdims=True) + base
        pos_row = jnp.sum(jnp.where(r0 < l0, jnp.broadcast_to(col_live, square), 0.0), axis=0, keepdims=True) + base
        one = jnp.where((ri == jnp.broadcast_to(pos_row, ri.shape))
                        & (jnp.broadcast_to(alive, ri.shape) == 1.0), 1.0, 0.0)
        sel[m // 2, :, (m % 2) * slots:(m % 2 + 1) * slots] = one.astype(BF16)
        tgt = tgt + jnp.sum(one * ti[m, 0].astype(F32), axis=1, keepdims=True)
        spots = jnp.where(col_live == 1.0, pos_col, -1.0)
        back[m] = jnp.where(li == jnp.broadcast_to(spots, li.shape), 1.0, 0.0).astype(BF16)
        base = base + jnp.sum(alive, axis=1, keepdims=True)
    live[...] = jnp.broadcast_to(base, live.shape)
    word = tgt - offset.astype(F32)
    meta[0] = jnp.broadcast_to(jnp.where((word >= 0.0) & (word < words), word, -1.0), lane)
    rl = lax.broadcasted_iota(jnp.int32, lane, 0).astype(F32)
    meta[1] = jnp.where(rl < jnp.broadcast_to(base, lane), 1.0, 0.0)
    sm[...] = jnp.zeros(lane, F32)

    def pass_on(c):
        first[c].wait_recv()
        piece = wv.at[half_rows(far, y), cols_at(c)]
        second.append(go(piece, piece, c_s.at[c], c_r.at[c], beside))
        cross.append(go(piece, piece, d_s.at[c], d_r.at[c], mate))

    def near_rows(c):
        nigh[c].wait_recv()
        buf[:, cols_at(c)] = jnp.dot(sel[x], wv[side_rows(x), cols_at(c)], preferred_element_type=F32).astype(BF16)

    def pass_mate(c):
        second[c].wait_recv()
        piece = wv.at[half_rows(far, 1 - y), cols_at(c)]
        third.append(go(piece, piece, e_s.at[c], e_r.at[c], mate))

    def far_rows(c):
        cross[c].wait_recv()
        third[c].wait_recv()
        h = jnp.dot(sel[far], wv[side_rows(far), cols_at(c)], preferred_element_type=F32)
        acc = sm[...]
        for k in range(tile // 128):
            at = c * tile + k * 128
            part = h[:, k * 128:(k + 1) * 128] + buf[:, at:at + 128].astype(F32)
            buf[:, at:at + 128] = part.astype(BF16)
            acc = acc + part * part
        sm[...] = acc

    for i in range(chunks + 3):
        for lag, f in ((0, pass_on), (0, near_rows), (2, pass_mate), (3, far_rows)):
            if 0 <= i - lag < chunks:
                f(i - lag)

    for cp in copies:
        cp.wait_send()
    copies.clear()
    edge = words // 16 * 16
    wv[edge:, :] = jnp.zeros((padded - edge, width), BF16)
    load(tiles - 1).start()
    mean = jnp.sum(sm[...], axis=1, keepdims=True) / width
    meta[2] = jnp.broadcast_to(lax.rsqrt(mean + EPSILON), lane)
    steps = width // (2 * tile)
    kb = tile // 128
    zrows = rows // nz
    spot = x * ny + y
    mine_rows = pl.ds(pl.multiple_of(z * zrows, 16), zrows)
    for s in range(steps):
        hsel[s] = buf[mine_rows, pl.ds(pl.multiple_of((2 * s + core) * tile + spot * 128, 128), 128)]

    def norm(c, carry):
        for k in range(tile // 128):
            cols = pl.ds(pl.multiple_of(c * tile + k * 128, 128), 128)
            buf[:, cols] = (buf[:, cols].astype(F32) * meta[2] * gain[:, cols]).astype(BF16)
        return carry
    lax.fori_loop(0, width // tile, norm, 0)

    mx[...] = jnp.full(lane, F_MIN, F32)
    tg[...] = jnp.zeros(lane, F32)
    sm[...] = jnp.zeros(lane, F32)

    def fold(t):
        for b in range(0, rows, 32):
            band = slice(b, b + 32)
            want = meta[0, band] - float(t * tile)
            old = mx[band]
            parts = [lg[band, t * tile + k * 128:t * tile + (k + 1) * 128] for k in range(tile // 128)]
            top = old
            for part in parts:
                top = jnp.maximum(top, part)
            hit = tg[band]
            acc = sm[band] * jnp.exp(old - top)
            for k, part in enumerate(parts):
                here = (lax.broadcasted_iota(jnp.int32, (1, 128), 1) + k * 128).astype(F32)
                hit = hit + jnp.where(want == here, part, 0.0)
                acc = acc + jnp.exp(part - top)
            mx[band] = top
            tg[band] = hit
            sm[band] = acc

    def multiply(t):
        wt = wv[t * tile:(t + 1) * tile, :]
        logit = lax.dot_general(buf[...], wt, (((1,), (1,)), ((), ())), preferred_element_type=F32)
        col = lax.broadcasted_iota(jnp.int32, (1, 128), 1)
        for k in range(tile // 128):
            part = logit[:, k * 128:(k + 1) * 128]
            first_word = t * tile + k * 128
            if first_word + 128 > words:
                part = jnp.where(col + first_word < words, part, F_MIN)
            lg[:, first_word:first_word + 128] = part

    for t in range(tiles):
        load(t).wait()
        if t:
            fold(t - 1)
        multiply(t)
    fold(tiles - 1)

    top = jnp.max(mx[...], axis=1, keepdims=True)
    hit = jnp.sum(tg[...], axis=1, keepdims=True)
    total = jnp.sum(sm[...] * jnp.exp(mx[...] - jnp.broadcast_to(top, lane)), axis=1, keepdims=True)
    part_lse = top + jnp.log(total)
    blk = 64
    groups = -(-rows // 128)
    st[...] = jnp.zeros(st.shape, F32)
    for i, piece in enumerate(lanes_of(jnp.broadcast_to(part_lse, lane))):
        st[i:i + 1, :] = piece
    stats = [go(st, box.at[j], st_s.at[j], st_r.at[j], t) for j, t in enumerate(peers)]
    st2[...] = jnp.zeros(st2.shape, F32)
    for i, piece in enumerate(lanes_of(jnp.broadcast_to(hit, lane))):
        st2[groups + i:groups + i + 1, :] = piece
    for cp in stats:
        cp.wait_recv()
    mine = st[...]
    best = jnp.maximum(mine, jnp.max(box[...], axis=0))
    total = jnp.exp(mine - best) + jnp.sum(jnp.exp(box[...] - best[None]), axis=0)
    lse = best + jnp.log(total)
    count = live[0:1, :]
    for i in range(groups):
        size = min(128, rows - i * 128)
        mx[i * 128:i * 128 + size] = jnp.broadcast_to(col_of(lse[i:i + 1], size), (size, 128))
    tg[...] = jnp.zeros(lane, F32)
    coef = scale_ref[0] / count

    def logit_grad(t, carry):
        for b in range(0, rows, blk):
            ref = mx[b:b + blk]
            factor = coef * meta[1, b:b + blk]
            want = meta[0, b:b + blk] - (t * tile).astype(F32)
            acc = tg[b:b + blk]
            for k in range(tile // 128):
                cols = pl.ds(pl.multiple_of(t * tile + k * 128, 128), 128)
                l = lg[b:b + blk, cols]
                here = (lax.broadcasted_iota(jnp.int32, (1, 128), 1) + k * 128).astype(F32)
                hot = jnp.where(want == here, 1.0, 0.0)
                g = ((jnp.exp(l - ref) - hot) * factor).astype(BF16)
                buf[b:b + blk, cols] = g
                acc = acc + g.astype(F32) * l
            tg[b:b + blk] = acc
        return carry
    lax.fori_loop(0, tiles, logit_grad, 0)
    for i, piece in enumerate(lanes_of(jnp.broadcast_to(jnp.sum(tg[...], axis=1, keepdims=True), lane))):
        st2[i:i + 1, :] = piece
    dots = [go(st2, box2.at[j], s2_s.at[j], s2_r.at[j], t) for j, t in enumerate(peers)]

    def ways(s):
        par = lax.rem(core + s, 2)
        found = []
        for a, b in ((1 - par, par), (par, 1 - par), (1, 1)):
            tx, ty = flip(x, a), flip(y, b)
            found.append(((tx * 2 + core, z * ny + ty), tx * ny + ty))
        return found
    along = [(p, lax.rem(z + d, nz) * ny + y) for d in range(1, nz)]
    to_mate, to_near, to_z, ag_z, ag_x, ag_m = {}, {}, {}, {}, {}, {}

    def product(j, slot):
        lg[:, slot * tile:(slot + 1) * tile] = jnp.dot(
            buf[:, :padded], wv[:, pl.ds(pl.multiple_of(j * tile, tile), tile)],
            preferred_element_type=F32)

    def for_mate(s):
        slot = 1 + s % 2
        if s >= 2:
            to_mate[s - 2].wait_send()
        product(2 * s + (1 - core), slot)
        to_mate[s] = remote(lg.at[:, slot * tile:(slot + 1) * tile], mr.at[s], m_s.at[s], m_r.at[s], mate)
        to_mate[s].start()

    def pair_sum(s, block):
        cols = pl.ds(pl.multiple_of(block * 128, 128), 128)
        return lg[:, cols] + mr[s, :, cols]

    def send_near(s, q, block, target):
        sb[s, q] = block.astype(BF16)
        to_near[s, q] = go(sb.at[s, q], rb.at[s, q], x_s.at[s, q], x_r.at[s, q], target)

    def for_self(s):
        product(2 * s + core, 0)
        to_mate[s].wait_recv()
        (one, b1), (two, b2), (opp, bd) = ways(s)
        send_near(s, 2, pair_sum(s, bd), opp)
        send_near(s, 0, pair_sum(s, b1), one)
        send_near(s, 1, pair_sum(s, b2), two)
        own[s] = pair_sum(s, spot)

    def plane(s):
        for q in range(3):
            to_near[s, q].wait_recv()
        own[s] = own[s] + (rb[s, 0].astype(F32) + rb[s, 1].astype(F32) + rb[s, 2].astype(F32))
        for d in range(1, nz):
            zz = lax.rem(z + d, nz)
            zs[s, d - 1] = own[s, pl.ds(pl.multiple_of(zz * zrows, 16), zrows)].astype(BF16)
            to_z[s, d] = go(zs.at[s, d - 1], zr.at[s, d - 1], z_s.at[s, d - 1], z_r.at[s, d - 1], along[d - 1])

    def row_dots():
        for cp in dots:
            cp.wait_recv()
        full = st2[...] + jnp.sum(box2[...], axis=0)
        missing = jnp.zeros((1, 128), F32)
        for i in range(groups):
            at = (lax.broadcasted_iota(jnp.int32, (1, 128), 1) + i * 128).astype(F32)
            missing = missing + jnp.where(at < count, lse[i:i + 1] - full[groups + i:groups + i + 1], 0.0)
        loss[0, 0] = jnp.sum(missing / count)
        for i in range(groups):
            size = min(128, rows - i * 128)
            tg[i * 128:i * 128 + size] = jnp.broadcast_to(col_of(full[i:i + 1], size), (size, 128))

    def finish(s):
        for d in range(1, nz):
            to_z[s, d].wait_recv()
        g = own[s, mine_rows]
        for d in range(1, nz):
            g = g + zr[s, d - 1].astype(F32)
        cols = pl.ds(pl.multiple_of((2 * s + core) * tile + spot * 128, 128), 128)
        r = meta[2, mine_rows]
        h = hsel[s].astype(F32)
        value = r * (gain[:, cols] * g) - (r * r) * h * (tg[mine_rows] * (1.0 / width))
        ag[core, spot, s, z] = value.astype(BF16)
        for d in range(1, nz):
            piece = ag.at[core, spot, s, z]
            ag_z[s, d] = go(piece, piece, az_s.at[s, d - 1], az_r.at[s, d - 1], along[d - 1])

    def send_plane(s, q, block, target):
        piece = ag.at[core, block, s]
        ag_x[s, q] = go(piece, piece, ax_s.at[s, q], ax_r.at[s, q], target)

    def send_mate(s, q, block):
        piece = ag.at[core, block, s]
        ag_m[s, q] = go(piece, piece, am_s.at[s, q], am_r.at[s, q], mate)

    def spread(s):
        for d in range(1, nz):
            ag_z[s, d].wait_recv()
        (one, b1), (two, b2), (opp, bd) = ways(s)
        send_plane(s, 0, spot, one)
        send_plane(s, 1, spot, two)
        send_plane(s, 2, spot, opp)
        send_mate(s, 3, spot)

    def share(s):
        for q, (target_id, block) in enumerate(ways(s)):
            ag_x[s, q].wait_recv()
            send_mate(s, q, block)

    def scatter(s):
        for q in range(4):
            ag_m[s, q].wait_recv()
        for c in range(2):
            block = jnp.concatenate([ag[c, k, s].reshape(rows, 128) for k in range(kb)], axis=1)
            res = jnp.dot(back[p], block, preferred_element_type=F32).astype(BF16)
            out[:, (2 * s + c) * tile:(2 * s + c + 1) * tile] = res

    for s in range(steps):
        for_mate(s)
        if s >= 3:
            plane(s - 3)
        for_self(s)
    row_dots()
    tail = []
    for i in range(steps + 6):
        for lag, f in ((0, plane), (1, finish), (2, spread), (3, share), (4, scatter)):
            s = i + steps - 3 - lag
            if 0 <= s < steps and not (f is plane and s <= steps - 4):
                tail.append((f, s))
    for f, s in tail:
        f(s)
    for s in range(max(steps - 2, 0), steps):
        to_mate[s].wait_send()
    for cp in copies:
        cp.wait_send()


def head(hidden, ints, norm_gain, out_weight, counts, loss_scale, pipe, vocab, ny):
    slots, width = hidden.shape
    rows = LIVE_SHARE * pipe
    words = out_weight.shape[0]
    padded = -(-words // 512) * 512
    nz = vocab // ny
    chunks = width // 512
    steps = width // 1024
    n = pipe * vocab - 1
    zrows = rows // nz
    dma = pltpu.SemaphoreType.DMA
    vm = pltpu.VMEM
    smem = pl.BlockSpec(memory_space=pltpu.SMEM)
    held = [pltpu.with_memory_space_constraint(a, pltpu.HBM)
            for a in (hidden, *ints, norm_gain.reshape(1, width), out_weight)]
    return pl.pallas_call(
        functools.partial(head_kernel, pipe, vocab, ny, words),
        out_shape=(
            jax.ShapeDtypeStruct((slots, width), BF16),
            jax.ShapeDtypeStruct((1, 1), F32),
        ),
        in_specs=[smem, smem] + [pl.BlockSpec(memory_space=pltpu.HBM)] * 6,
        out_specs=(VMEM, smem),
        scratch_shapes=[
            vm((padded, width), BF16),
            vm((rows, padded), F32),
            vm((rows, max(padded, width)), BF16),
            vm((2, rows, 2 * slots), BF16),
            vm((pipe, slots, rows), BF16),
            vm((pipe, 3, 1, slots), jnp.int32),
            vm((1, width), F32),
            vm((3, rows, 128), F32),
            vm((8, 128), F32),
            vm((steps, zrows, 128), BF16),
            vm((rows, 128), F32), vm((rows, 128), F32), vm((rows, 128), F32),
            vm((4, 128), F32), vm((n, 4, 128), F32),
            vm((8, 128), F32), vm((n, 8, 128), F32),
            vm((steps, rows, 512), F32),
            vm((steps, 3, rows, 128), BF16),
            vm((steps, 3, rows, 128), BF16),
            vm((steps, rows, 128), F32),
            vm((steps, nz - 1, zrows, 128), BF16),
            vm((steps, nz - 1, zrows, 128), BF16),
            vm((2, 4, steps, nz, zrows, 128), BF16),
            dma((padded // 512,)), dma((chunks,)), dma((4,)),
            dma((chunks,)), dma((chunks,)), dma((chunks,)), dma((chunks,)),
            dma((chunks,)), dma((chunks,)), dma((chunks,)), dma((chunks,)),
            dma((chunks,)), dma((chunks,)), dma((3,)), dma((3,)),
            dma((n,)), dma((n,)), dma((n,)), dma((n,)),
            dma((steps,)), dma((steps,)),
            dma((steps, 3)), dma((steps, 3)),
            dma((steps, nz - 1)), dma((steps, nz - 1)),
            dma((steps, nz - 1)), dma((steps, nz - 1)),
            dma((steps, 3)), dma((steps, 3)),
            dma((steps, 4)), dma((steps, 4)),
        ],
        compiler_params=pltpu.CompilerParams(
            collective_id=0, has_side_effects=True, vmem_limit_bytes=52 * 2**20
        ),
    )(counts, loss_scale.reshape(1), *held)


def body(pipe, vocab, hidden, norm_gain, out_weight, targets, loss_mask, slot_position, counts, loss_scale):
    micro_slots = hidden.shape[1]
    model_width = hidden.shape[2]
    shard_words = out_weight.shape[0]
    ny = 2
    nz = vocab // ny
    fast = (pipe == 4 and vocab == 8 and micro_slots == 128 and micro_slots * pipe == 512 and model_width % 1024 == 0
            and shard_words % 8 == 0)
    if fast:
        grad_out, loss = head(
            hidden.reshape(micro_slots, model_width), (targets, loss_mask, slot_position),
            norm_gain, out_weight, counts, loss_scale, pipe, vocab, ny)
        return (loss[0, 0], grad_out.reshape(1, micro_slots, model_width))
    own_ints = jnp.concatenate(
        [targets, loss_mask, slot_position, jnp.zeros((5, micro_slots), jnp.int32)], axis=0
    )
    offset = lax.axis_index(("pipe", "vocab")) * shard_words
    own_rows = hidden.reshape(micro_slots, model_width).astype(F32)
    own_normed = rms_scale(own_rows, norm_gain).astype(BF16)
    all_normed = lax.all_gather(own_normed, "pipe", axis=0, tiled=True)
    all_ints = lax.all_gather(own_ints, "pipe", axis=0)
    rows_total = all_normed.shape[0]
    all_targets, all_masks, all_positions = (
        all_ints[:, k].reshape(rows_total) for k in range(3)
    )
    count_row = jnp.broadcast_to(counts[:, None], (counts.shape[0], micro_slots)).reshape(rows_total)
    inside = all_positions < count_row
    token_weight = jnp.where(inside & (all_masks == 1), 1.0, 0.0).astype(F32)
    weight_total = jnp.sum(token_weight)
    logits = lax.dot_general(
        all_normed, out_weight, (((1,), (1,)), ((), ())), preferred_element_type=F32
    )
    is_target = (
        jnp.arange(shard_words, dtype=jnp.int32)[None, :] == (all_targets - offset)[:, None]
    )
    local_target = jnp.sum(jnp.where(is_target, logits, 0.0), axis=1)
    local_top = jnp.max(logits, axis=1)
    row_top = lax.pmax(local_top, ("pipe", "vocab"))
    local_total = jnp.sum(jnp.exp(logits - row_top[:, None]), axis=1)
    exp_total, target_logit = lax.psum((local_total, local_target), ("pipe", "vocab"))
    log_total = row_top + jnp.log(exp_total)
    loss = jnp.sum(token_weight * (log_total - target_logit)) / weight_total
    token_coef = loss_scale * token_weight / weight_total
    logit_grad = (
        (jnp.exp(logits - log_total[:, None]) - is_target.astype(F32)) * token_coef[:, None]
    ).astype(BF16)
    work_grad = jnp.dot(logit_grad, out_weight, preferred_element_type=F32)
    grad_cube = work_grad.reshape(rows_total // micro_slots, micro_slots, model_width)
    micro_grad = lax.psum_scatter(grad_cube, "pipe", scatter_dimension=0, tiled=True)
    summed = lax.psum(micro_grad, "vocab")
    grad_out = pull_rows(own_rows, norm_gain, summed.reshape(micro_slots, model_width))
    return (loss, grad_out.reshape(1, micro_slots, model_width))


def solution(mesh):
    in_specs = (
        P("pipe", None, None),
        P(),
        P(("pipe", "vocab"), None),
        P("pipe", None),
        P("pipe", None),
        P("pipe", None),
        P(),
        P(),
    )
    out_specs = (P(), P("pipe", None, None))
    part = functools.partial(body, mesh.shape["pipe"], mesh.shape["vocab"])
    return jax.shard_map(part, mesh=mesh, in_specs=in_specs, out_specs=out_specs, check_vma=False)
```

```python
import functools
import jax
import jax.numpy as jnp
from jax import lax
from jax.experimental import pallas as pl
from jax.experimental.pallas import tpu as pltpu
from jax.sharding import PartitionSpec as P

EPSILON = 1e-05
MESH = pl.DeviceIdType.MESH
F32 = jnp.float32
BF16 = jnp.bfloat16
VMEM = pl.BlockSpec(memory_space=pltpu.VMEM)


def rms_scale(values, norm_gain):
    mean_square = jnp.mean(values * values, axis=-1, keepdims=True)
    return values * lax.rsqrt(mean_square + EPSILON) * norm_gain


def pull_rows(rows, norm_gain, cotangent):
    pullback = jax.vjp(lambda values: rms_scale(values, norm_gain), rows)[1]
    return pullback(cotangent)[0].astype(BF16)


def place(ny):
    p, v = lax.axis_index("pipe"), lax.axis_index("vocab")
    return p // 2, p % 2, v % ny, v // ny


def greet(targets):
    barrier = pltpu.get_barrier_semaphore()
    for target in targets:
        pl.semaphore_signal(barrier, inc=1, device_id=target, device_id_type=MESH)
    pl.semaphore_wait(barrier, len(targets))


def remote(src, dst, send, recv, target):
    return pltpu.make_async_remote_copy(
        src_ref=src, dst_ref=dst, send_sem=send, recv_sem=recv,
        device_id=target, device_id_type=MESH,
    )


LIVE_SHARE = 80
F_MIN = -1e30


def flip(i, by):
    return i + by * (1 - 2 * i)


def lanes_of(col):
    rows, lanes = col.shape
    outs = []
    for b in range(0, rows, lanes):
        part = col[b:min(b + lanes, rows)]
        r = lax.broadcasted_iota(jnp.int32, part.shape, 0)
        l = lax.broadcasted_iota(jnp.int32, part.shape, 1)
        outs.append(jnp.sum(jnp.where(r == l, part, 0.0), axis=0, keepdims=True))
    return outs


def col_of(row, count):
    shape = (count, row.shape[1])
    r = lax.broadcasted_iota(jnp.int32, shape, 0)
    l = lax.broadcasted_iota(jnp.int32, shape, 1)
    return jnp.sum(jnp.where(r == l, jnp.broadcast_to(row, shape), 0.0), axis=1, keepdims=True)


def head_kernel(pipe, vocab, ny, words, counts, scale_ref, hidden, targets, masks, places, gain_hbm, weight,
                out, loss, wv, lg, buf, sel, back, ti, gain, meta, live, hsel, mx, tg, sm,
                st, box, st2, box2, mr, sb, rb, own, zs, zr, ag,
                ready, w_sem, o_sem, i_sem, f_s, f_r, n_s, n_r, c_s, c_r, d_s, d_r, e_s, e_r, t_s, t_r,
                st_s, st_r, s2_s, s2_r, m_s, m_r, x_s, x_r, z_s, z_r, az_s, az_r,
                ax_s, ax_r, am_s, am_r):
    x, core, y, z = place(ny)
    p, v = x * 2 + core, z * ny + y
    nz = vocab // ny
    slots, width = hidden.shape
    half = slots // 2
    rows = buf.shape[0]
    padded = wv.shape[0]
    tile = 512
    tiles = padded // tile
    rest = words - (tiles - 1) * tile
    lane = (rows, 128)
    offset = (p * vocab + v) * words
    chunks = width // tile
    far = 1 - x
    mate = (x * 2 + (1 - core), v)
    across = ((1 - x) * 2 + core, v)
    diag = ((1 - x) * 2 + (1 - core), v)
    beside = (p, z * ny + (1 - y))
    copies = []

    def go(src, dst, send, recv, target):
        cp = remote(src, dst, send, recv, target)
        cp.start()
        copies.append(cp)
        return cp

    def cols_at(c):
        return pl.ds(c * tile, tile)

    pool = (tiles - 1) * tile

    def half_rows(a, side):
        return pl.ds(pl.multiple_of(pool + (a * 2 + core) * slots + side * half, half), half)

    def side_rows(a):
        return pl.ds(pl.multiple_of(pool + a * 2 * slots, slots), 2 * slots)

    all_rows = pl.ds(pl.multiple_of(pool + p * slots, slots), slots)
    bring = [pltpu.make_async_copy(hidden.at[:, cols_at(c)], wv.at[all_rows, cols_at(c)], o_sem.at[c])
             for c in range(chunks)]
    small = [pltpu.make_async_copy(src, ti.at[p, k], i_sem.at[k])
             for k, src in enumerate((targets, masks, places))]
    small.append(pltpu.make_async_copy(gain_hbm, gain, i_sem.at[3]))
    for cp in small + bring:
        cp.start()

    def load(t):
        size = tile if t < tiles - 1 else rest
        return pltpu.make_async_copy(
            weight.at[pl.ds(t * tile, size)], wv.at[pl.ds(t * tile, size)], w_sem.at[t])

    peers = []
    for dp in range(pipe):
        for dv in range(vocab):
            if dp or dv:
                peers.append((lax.rem(p + dp, pipe), lax.rem(v + dv, vocab)))
    close = [mate, across, diag, beside]
    inner = (z > 0).astype(jnp.int32) + (z < nz - 1).astype(jnp.int32)

    def call_column(sem):
        @pl.when(z > 0)
        def _():
            pl.semaphore_signal(sem, inc=1, device_id=(p, v - ny), device_id_type=MESH)

        @pl.when(z < nz - 1)
        def _():
            pl.semaphore_signal(sem, inc=1, device_id=(p, v + ny), device_id_type=MESH)

    def call_close(sem):
        for target in close:
            pl.semaphore_signal(sem, inc=1, device_id=target, device_id_type=MESH)

    entry = pltpu.get_barrier_semaphore()
    call_close(entry)
    call_column(entry)
    pl.semaphore_wait(entry, inner + len(close))

    for cp in small:
        cp.wait()
    info = [go(ti.at[p], ti.at[p], t_s.at[j], t_r.at[j], target)
            for j, target in enumerate((mate, across, diag))]
    first, nigh, cross, second, third = [], [], [], [], []
    for c in range(chunks):
        bring[c].wait()
        piece = wv.at[half_rows(x, y), cols_at(c)]
        first.append(go(piece, piece, f_s.at[c], f_r.at[c], across))
        piece = wv.at[all_rows, cols_at(c)]
        nigh.append(go(piece, piece, n_s.at[c], n_r.at[c], mate))
    for t in range(tiles - 1):
        load(t).start()
    call_column(ready.at[0])
    pl.semaphore_wait(ready.at[0], inner)
    call_column(ready.at[1])
    for cp in info:
        cp.wait_recv()

    square = (slots, slots)
    r0 = lax.broadcasted_iota(jnp.int32, square, 0)
    l0 = lax.broadcasted_iota(jnp.int32, square, 1)
    ri = lax.broadcasted_iota(jnp.int32, (rows, slots), 0).astype(F32)
    li = lax.broadcasted_iota(jnp.int32, (slots, rows), 1).astype(F32)
    base = jnp.zeros((1, 1), F32)
    tgt = jnp.zeros((rows, 1), F32)
    for m in range(pipe):
        inside = ti[m, 2] < counts[m]
        alive = jnp.where(inside & (ti[m, 1] == 1), 1.0, 0.0).astype(F32)
        alive_sq = jnp.broadcast_to(alive, square)
        col_live = jnp.sum(jnp.where(r0 == l0, alive_sq, 0.0), axis=1, keepdims=True)
        pos_col = jnp.sum(jnp.where(l0 < r0, alive_sq, 0.0), axis=1, keepdims=True) + base
        pos_row = jnp.sum(jnp.where(r0 < l0, jnp.broadcast_to(col_live, square), 0.0), axis=0, keepdims=True) + base
        one = jnp.where((ri == jnp.broadcast_to(pos_row, ri.shape))
                        & (jnp.broadcast_to(alive, ri.shape) == 1.0), 1.0, 0.0)
        sel[m // 2, :, (m % 2) * slots:(m % 2 + 1) * slots] = one.astype(BF16)
        tgt = tgt + jnp.sum(one * ti[m, 0].astype(F32), axis=1, keepdims=True)
        spots = jnp.where(col_live == 1.0, pos_col, -1.0)
        back[m] = jnp.where(li == jnp.broadcast_to(spots, li.shape), 1.0, 0.0).astype(BF16)
        base = base + jnp.sum(alive, axis=1, keepdims=True)
    live[...] = jnp.broadcast_to(base, live.shape)
    pl.semaphore_wait(ready.at[1], inner)
    call_close(ready.at[2])
    word = tgt - offset.astype(F32)
    meta[0] = jnp.broadcast_to(jnp.where((word >= 0.0) & (word < words), word, -1.0), lane)
    rl = lax.broadcasted_iota(jnp.int32, lane, 0).astype(F32)
    meta[1] = jnp.where(rl < jnp.broadcast_to(base, lane), 1.0, 0.0)
    sm[...] = jnp.zeros(lane, F32)

    def pass_on(c):
        first[c].wait_recv()
        piece = wv.at[half_rows(far, y), cols_at(c)]
        second.append(go(piece, piece, c_s.at[c], c_r.at[c], beside))
        cross.append(go(piece, piece, d_s.at[c], d_r.at[c], mate))

    def near_rows(c):
        nigh[c].wait_recv()
        buf[:, cols_at(c)] = jnp.dot(sel[x], wv[side_rows(x), cols_at(c)], preferred_element_type=F32).astype(BF16)

    def pass_mate(c):
        second[c].wait_recv()
        piece = wv.at[half_rows(far, 1 - y), cols_at(c)]
        third.append(go(piece, piece, e_s.at[c], e_r.at[c], mate))

    def far_rows(c):
        cross[c].wait_recv()
        third[c].wait_recv()
        h = jnp.dot(sel[far], wv[side_rows(far), cols_at(c)], preferred_element_type=F32)
        acc = sm[...]
        for k in range(tile // 128):
            at = c * tile + k * 128
            part = h[:, k * 128:(k + 1) * 128] + buf[:, at:at + 128].astype(F32)
            buf[:, at:at + 128] = part.astype(BF16)
            acc = acc + part * part
        sm[...] = acc

    for i in range(chunks + 3):
        if i == 3:
            pl.semaphore_wait(ready.at[2], len(close))
            call_close(ready.at[3])
        if i == 6:
            pl.semaphore_wait(ready.at[3], len(close))
        for lag, f in ((0, pass_on), (0, near_rows), (2, pass_mate), (3, far_rows)):
            if 0 <= i - lag < chunks:
                f(i - lag)

    for cp in copies:
        cp.wait_send()
    copies.clear()
    edge = words // 16 * 16
    wv[edge:, :] = jnp.zeros((padded - edge, width), BF16)
    load(tiles - 1).start()
    mean = jnp.sum(sm[...], axis=1, keepdims=True) / width
    meta[2] = jnp.broadcast_to(lax.rsqrt(mean + EPSILON), lane)
    steps = width // (2 * tile)
    kb = tile // 128
    zrows = rows // nz
    spot = x * ny + y
    mine_rows = pl.ds(pl.multiple_of(z * zrows, 16), zrows)
    for s in range(steps):
        hsel[s] = buf[mine_rows, pl.ds(pl.multiple_of((2 * s + core) * tile + spot * 128, 128), 128)]

    def norm(c, carry):
        for k in range(tile // 128):
            cols = pl.ds(pl.multiple_of(c * tile + k * 128, 128), 128)
            buf[:, cols] = (buf[:, cols].astype(F32) * meta[2] * gain[:, cols]).astype(BF16)
        return carry
    lax.fori_loop(0, width // tile, norm, 0)

    mx[...] = jnp.full(lane, F_MIN, F32)
    tg[...] = jnp.zeros(lane, F32)
    sm[...] = jnp.zeros(lane, F32)

    def fold(t):
        for b in range(0, rows, 32):
            band = slice(b, b + 32)
            want = meta[0, band] - float(t * tile)
            old = mx[band]
            parts = [lg[band, t * tile + k * 128:t * tile + (k + 1) * 128] for k in range(tile // 128)]
            top = old
            for part in parts:
                top = jnp.maximum(top, part)
            hit = tg[band]
            acc = sm[band] * jnp.exp(old - top)
            for k, part in enumerate(parts):
                here = (lax.broadcasted_iota(jnp.int32, (1, 128), 1) + k * 128).astype(F32)
                hit = hit + jnp.where(want == here, part, 0.0)
                acc = acc + jnp.exp(part - top)
            mx[band] = top
            tg[band] = hit
            sm[band] = acc

    def multiply(t):
        wt = wv[t * tile:(t + 1) * tile, :]
        logit = lax.dot_general(buf[...], wt, (((1,), (1,)), ((), ())), preferred_element_type=F32)
        col = lax.broadcasted_iota(jnp.int32, (1, 128), 1)
        for k in range(tile // 128):
            part = logit[:, k * 128:(k + 1) * 128]
            first_word = t * tile + k * 128
            if first_word + 128 > words:
                part = jnp.where(col + first_word < words, part, F_MIN)
            lg[:, first_word:first_word + 128] = part

    for t in range(tiles):
        load(t).wait()
        if t:
            fold(t - 1)
        multiply(t)
    fold(tiles - 1)

    top = jnp.max(mx[...], axis=1, keepdims=True)
    hit = jnp.sum(tg[...], axis=1, keepdims=True)
    total = jnp.sum(sm[...] * jnp.exp(mx[...] - jnp.broadcast_to(top, lane)), axis=1, keepdims=True)
    part_lse = top + jnp.log(total)
    blk = 64
    groups = -(-rows // 128)
    st[...] = jnp.zeros(st.shape, F32)
    for i, piece in enumerate(lanes_of(jnp.broadcast_to(part_lse, lane))):
        st[i:i + 1, :] = piece
    stats = [go(st, box.at[j], st_s.at[j], st_r.at[j], t) for j, t in enumerate(peers)]
    st2[...] = jnp.zeros(st2.shape, F32)
    for i, piece in enumerate(lanes_of(jnp.broadcast_to(hit, lane))):
        st2[groups + i:groups + i + 1, :] = piece
    for cp in stats:
        cp.wait_recv()
    mine = st[...]
    best = jnp.maximum(mine, jnp.max(box[...], axis=0))
    total = jnp.exp(mine - best) + jnp.sum(jnp.exp(box[...] - best[None]), axis=0)
    lse = best + jnp.log(total)
    count = live[0:1, :]
    for i in range(groups):
        size = min(128, rows - i * 128)
        mx[i * 128:i * 128 + size] = jnp.broadcast_to(col_of(lse[i:i + 1], size), (size, 128))
    tg[...] = jnp.zeros(lane, F32)
    coef = scale_ref[0] / count

    def logit_grad(t, carry):
        for b in range(0, rows, blk):
            ref = mx[b:b + blk]
            factor = coef * meta[1, b:b + blk]
            want = meta[0, b:b + blk] - (t * tile).astype(F32)
            acc = tg[b:b + blk]
            for k in range(tile // 128):
                cols = pl.ds(pl.multiple_of(t * tile + k * 128, 128), 128)
                l = lg[b:b + blk, cols]
                here = (lax.broadcasted_iota(jnp.int32, (1, 128), 1) + k * 128).astype(F32)
                hot = jnp.where(want == here, 1.0, 0.0)
                g = ((jnp.exp(l - ref) - hot) * factor).astype(BF16)
                buf[b:b + blk, cols] = g
                acc = acc + g.astype(F32) * l
            tg[b:b + blk] = acc
        return carry
    lax.fori_loop(0, tiles, logit_grad, 0)
    for i, piece in enumerate(lanes_of(jnp.broadcast_to(jnp.sum(tg[...], axis=1, keepdims=True), lane))):
        st2[i:i + 1, :] = piece
    dots = [go(st2, box2.at[j], s2_s.at[j], s2_r.at[j], t) for j, t in enumerate(peers)]

    def ways(s):
        par = lax.rem(core + s, 2)
        found = []
        for a, b in ((1 - par, par), (par, 1 - par), (1, 1)):
            tx, ty = flip(x, a), flip(y, b)
            found.append(((tx * 2 + core, z * ny + ty), tx * ny + ty))
        return found
    along = [(p, lax.rem(z + d, nz) * ny + y) for d in range(1, nz)]
    to_mate, to_near, to_z, ag_z, ag_x, ag_m = {}, {}, {}, {}, {}, {}

    def product(j, slot):
        lg[:, slot * tile:(slot + 1) * tile] = jnp.dot(
            buf[:, :padded], wv[:, pl.ds(pl.multiple_of(j * tile, tile), tile)],
            preferred_element_type=F32)

    def for_mate(s):
        slot = 1 + s % 2
        if s >= 2:
            to_mate[s - 2].wait_send()
        product(2 * s + (1 - core), slot)
        to_mate[s] = remote(lg.at[:, slot * tile:(slot + 1) * tile], mr.at[s], m_s.at[s], m_r.at[s], mate)
        to_mate[s].start()

    def pair_sum(s, block):
        cols = pl.ds(pl.multiple_of(block * 128, 128), 128)
        return lg[:, cols] + mr[s, :, cols]

    def send_near(s, q, block, target):
        sb[s, q] = block.astype(BF16)
        to_near[s, q] = go(sb.at[s, q], rb.at[s, q], x_s.at[s, q], x_r.at[s, q], target)

    def for_self(s):
        product(2 * s + core, 0)
        to_mate[s].wait_recv()
        (one, b1), (two, b2), (opp, bd) = ways(s)
        send_near(s, 2, pair_sum(s, bd), opp)
        send_near(s, 0, pair_sum(s, b1), one)
        send_near(s, 1, pair_sum(s, b2), two)
        own[s] = pair_sum(s, spot)

    def plane(s):
        for q in range(3):
            to_near[s, q].wait_recv()
        own[s] = own[s] + (rb[s, 0].astype(F32) + rb[s, 1].astype(F32) + rb[s, 2].astype(F32))
        for d in range(1, nz):
            zz = lax.rem(z + d, nz)
            zs[s, d - 1] = own[s, pl.ds(pl.multiple_of(zz * zrows, 16), zrows)].astype(BF16)
            to_z[s, d] = go(zs.at[s, d - 1], zr.at[s, d - 1], z_s.at[s, d - 1], z_r.at[s, d - 1], along[d - 1])

    def row_dots():
        for cp in dots:
            cp.wait_recv()
        full = st2[...] + jnp.sum(box2[...], axis=0)
        missing = jnp.zeros((1, 128), F32)
        for i in range(groups):
            at = (lax.broadcasted_iota(jnp.int32, (1, 128), 1) + i * 128).astype(F32)
            missing = missing + jnp.where(at < count, lse[i:i + 1] - full[groups + i:groups + i + 1], 0.0)
        loss[0, 0] = jnp.sum(missing / count)
        for i in range(groups):
            size = min(128, rows - i * 128)
            tg[i * 128:i * 128 + size] = jnp.broadcast_to(col_of(full[i:i + 1], size), (size, 128))

    def finish(s):
        for d in range(1, nz):
            to_z[s, d].wait_recv()
        g = own[s, mine_rows]
        for d in range(1, nz):
            g = g + zr[s, d - 1].astype(F32)
        cols = pl.ds(pl.multiple_of((2 * s + core) * tile + spot * 128, 128), 128)
        r = meta[2, mine_rows]
        h = hsel[s].astype(F32)
        value = r * (gain[:, cols] * g) - (r * r) * h * (tg[mine_rows] * (1.0 / width))
        ag[core, spot, s, z] = value.astype(BF16)
        for d in range(1, nz):
            piece = ag.at[core, spot, s, z]
            ag_z[s, d] = go(piece, piece, az_s.at[s, d - 1], az_r.at[s, d - 1], along[d - 1])

    def send_plane(s, q, block, target):
        piece = ag.at[core, block, s]
        ag_x[s, q] = go(piece, piece, ax_s.at[s, q], ax_r.at[s, q], target)

    def send_mate(s, q, block):
        piece = ag.at[core, block, s]
        ag_m[s, q] = go(piece, piece, am_s.at[s, q], am_r.at[s, q], mate)

    def spread(s):
        for d in range(1, nz):
            ag_z[s, d].wait_recv()
        (one, b1), (two, b2), (opp, bd) = ways(s)
        send_plane(s, 0, spot, one)
        send_plane(s, 1, spot, two)
        send_plane(s, 2, spot, opp)
        send_mate(s, 3, spot)

    def share(s):
        for q, (target_id, block) in enumerate(ways(s)):
            ag_x[s, q].wait_recv()
            send_mate(s, q, block)

    def scatter(s):
        for q in range(4):
            ag_m[s, q].wait_recv()
        for c in range(2):
            block = jnp.concatenate([ag[c, k, s].reshape(rows, 128) for k in range(kb)], axis=1)
            res = jnp.dot(back[p], block, preferred_element_type=F32).astype(BF16)
            out[:, (2 * s + c) * tile:(2 * s + c + 1) * tile] = res

    for s in range(steps):
        for_mate(s)
        if s >= 3:
            plane(s - 3)
        for_self(s)
    row_dots()
    tail = []
    for i in range(steps + 6):
        for lag, f in ((0, plane), (1, finish), (2, spread), (3, share), (4, scatter)):
            s = i + steps - 3 - lag
            if 0 <= s < steps and not (f is plane and s <= steps - 4):
                tail.append((f, s))
    for f, s in tail:
        f(s)
    for s in range(max(steps - 2, 0), steps):
        to_mate[s].wait_send()
    for cp in copies:
        cp.wait_send()


def head(hidden, ints, norm_gain, out_weight, counts, loss_scale, pipe, vocab, ny):
    slots, width = hidden.shape
    rows = LIVE_SHARE * pipe
    words = out_weight.shape[0]
    padded = -(-words // 512) * 512
    nz = vocab // ny
    chunks = width // 512
    steps = width // 1024
    n = pipe * vocab - 1
    zrows = rows // nz
    dma = pltpu.SemaphoreType.DMA
    vm = pltpu.VMEM
    smem = pl.BlockSpec(memory_space=pltpu.SMEM)
    held = [pltpu.with_memory_space_constraint(a, pltpu.HBM)
            for a in (hidden, *ints, norm_gain.reshape(1, width), out_weight)]
    return pl.pallas_call(
        functools.partial(head_kernel, pipe, vocab, ny, words),
        out_shape=(
            jax.ShapeDtypeStruct((slots, width), BF16),
            jax.ShapeDtypeStruct((1, 1), F32),
        ),
        in_specs=[smem, smem] + [pl.BlockSpec(memory_space=pltpu.HBM)] * 6,
        out_specs=(VMEM, smem),
        scratch_shapes=[
            vm((padded, width), BF16),
            vm((rows, padded), F32),
            vm((rows, max(padded, width)), BF16),
            vm((2, rows, 2 * slots), BF16),
            vm((pipe, slots, rows), BF16),
            vm((pipe, 3, 1, slots), jnp.int32),
            vm((1, width), F32),
            vm((3, rows, 128), F32),
            vm((8, 128), F32),
            vm((steps, zrows, 128), BF16),
            vm((rows, 128), F32), vm((rows, 128), F32), vm((rows, 128), F32),
            vm((4, 128), F32), vm((n, 4, 128), F32),
            vm((8, 128), F32), vm((n, 8, 128), F32),
            vm((steps, rows, 512), F32),
            vm((steps, 3, rows, 128), BF16),
            vm((steps, 3, rows, 128), BF16),
            vm((steps, rows, 128), F32),
            vm((steps, nz - 1, zrows, 128), BF16),
            vm((steps, nz - 1, zrows, 128), BF16),
            vm((2, 4, steps, nz, zrows, 128), BF16),
            pltpu.SemaphoreType.REGULAR((4,)), dma((padded // 512,)), dma((chunks,)), dma((4,)),
            dma((chunks,)), dma((chunks,)), dma((chunks,)), dma((chunks,)),
            dma((chunks,)), dma((chunks,)), dma((chunks,)), dma((chunks,)),
            dma((chunks,)), dma((chunks,)), dma((3,)), dma((3,)),
            dma((n,)), dma((n,)), dma((n,)), dma((n,)),
            dma((steps,)), dma((steps,)),
            dma((steps, 3)), dma((steps, 3)),
            dma((steps, nz - 1)), dma((steps, nz - 1)),
            dma((steps, nz - 1)), dma((steps, nz - 1)),
            dma((steps, 3)), dma((steps, 3)),
            dma((steps, 4)), dma((steps, 4)),
        ],
        compiler_params=pltpu.CompilerParams(
            collective_id=0, has_side_effects=True, vmem_limit_bytes=52 * 2**20
        ),
    )(counts, loss_scale.reshape(1), *held)


def body(pipe, vocab, hidden, norm_gain, out_weight, targets, loss_mask, slot_position, counts, loss_scale):
    micro_slots = hidden.shape[1]
    model_width = hidden.shape[2]
    shard_words = out_weight.shape[0]
    ny = 2
    nz = vocab // ny
    fast = (pipe == 4 and vocab == 8 and micro_slots == 128 and micro_slots * pipe == 512 and model_width % 1024 == 0
            and shard_words % 8 == 0)
    if fast:
        grad_out, loss = head(
            hidden.reshape(micro_slots, model_width), (targets, loss_mask, slot_position),
            norm_gain, out_weight, counts, loss_scale, pipe, vocab, ny)
        return (loss[0, 0], grad_out.reshape(1, micro_slots, model_width))
    own_ints = jnp.concatenate(
        [targets, loss_mask, slot_position, jnp.zeros((5, micro_slots), jnp.int32)], axis=0
    )
    offset = lax.axis_index(("pipe", "vocab")) * shard_words
    own_rows = hidden.reshape(micro_slots, model_width).astype(F32)
    own_normed = rms_scale(own_rows, norm_gain).astype(BF16)
    all_normed = lax.all_gather(own_normed, "pipe", axis=0, tiled=True)
    all_ints = lax.all_gather(own_ints, "pipe", axis=0)
    rows_total = all_normed.shape[0]
    all_targets, all_masks, all_positions = (
        all_ints[:, k].reshape(rows_total) for k in range(3)
    )
    count_row = jnp.broadcast_to(counts[:, None], (counts.shape[0], micro_slots)).reshape(rows_total)
    inside = all_positions < count_row
    token_weight = jnp.where(inside & (all_masks == 1), 1.0, 0.0).astype(F32)
    weight_total = jnp.sum(token_weight)
    logits = lax.dot_general(
        all_normed, out_weight, (((1,), (1,)), ((), ())), preferred_element_type=F32
    )
    is_target = (
        jnp.arange(shard_words, dtype=jnp.int32)[None, :] == (all_targets - offset)[:, None]
    )
    local_target = jnp.sum(jnp.where(is_target, logits, 0.0), axis=1)
    local_top = jnp.max(logits, axis=1)
    row_top = lax.pmax(local_top, ("pipe", "vocab"))
    local_total = jnp.sum(jnp.exp(logits - row_top[:, None]), axis=1)
    exp_total, target_logit = lax.psum((local_total, local_target), ("pipe", "vocab"))
    log_total = row_top + jnp.log(exp_total)
    loss = jnp.sum(token_weight * (log_total - target_logit)) / weight_total
    token_coef = loss_scale * token_weight / weight_total
    logit_grad = (
        (jnp.exp(logits - log_total[:, None]) - is_target.astype(F32)) * token_coef[:, None]
    ).astype(BF16)
    work_grad = jnp.dot(logit_grad, out_weight, preferred_element_type=F32)
    grad_cube = work_grad.reshape(rows_total // micro_slots, micro_slots, model_width)
    micro_grad = lax.psum_scatter(grad_cube, "pipe", scatter_dimension=0, tiled=True)
    summed = lax.psum(micro_grad, "vocab")
    grad_out = pull_rows(own_rows, norm_gain, summed.reshape(micro_slots, model_width))
    return (loss, grad_out.reshape(1, micro_slots, model_width))


def solution(mesh):
    in_specs = (
        P("pipe", None, None),
        P(),
        P(("pipe", "vocab"), None),
        P("pipe", None),
        P("pipe", None),
        P("pipe", None),
        P(),
        P(),
    )
    out_specs = (P(), P("pipe", None, None))
    part = functools.partial(body, mesh.shape["pipe"], mesh.shape["vocab"])
    return jax.shard_map(part, mesh=mesh, in_specs=in_specs, out_specs=out_specs, check_vma=False)
```
